512 devices in a mesh: groups: 2 (over y), rows: 16 (over z), sub: 8 (over x), pair: 2 (over core).
Axes of the slice: x: 8, y: 2, z: 16, core: 2. Of those that a mesh axis runs over, the one named last changes fastest.
The devices are a block of a 8x8x16 slice.
Arguments:
- embeddings: bfloat16 [131072, 1024], P(('groups', 'rows', 'sub', 'pair')), parts along dimension 0, may hold values from -80 to 80
- assignment: int32 [131072], P(('groups', 'rows', 'sub', 'pair')), parts along dimension 0, may hold values from 0 to 1023, as said below
- order: int32 [131072], P(('groups', 'rows', 'sub', 'pair')), parts along dimension 0, may hold values from 0 to 65535, each once
Outputs:
- max_similarity: float32 [131072], P(('groups', 'rows', 'sub', 'pair')), parts along dimension 0
- centre_distance: float32 [131072], P(('groups', 'rows', 'sub', 'pair')), parts along dimension 0
The draws below stay inside these ranges and needn't reach their ends.
There are 2 independent parts, one for each index of `groups`. The reference program is written for one: setup_inputs(seed, part) draws one part's arguments, and reference() takes and returns one part's arrays. A program takes and returns all parts, laid end to end along the dimension named above; each array names one. Nothing has to cross between parts.
Inputs may be any that keep to these rules, and one draw needn't show every extreme that they name: `assignment`: cluster c belongs to owner c // 8, owners being numbered along rows then sub. In each aligned block of 256 rows (the rows of one device) at most 8 rows name clusters of one owner, and one owner receives exactly 8 from every block; no cluster is named more than 1 times in one block.
All inputs are finite; a program needn't handle non-finite values.
Results may differ from the reference program's by a relative error of at most 0.00063.
Values may be sent and summed in bfloat16 or wider, within the bound.
A program may use at most 64 MiB of HBM per device.

```python
import jax
import jax.numpy as jnp
from jax import lax

D = 1024
K = 1024
ROW_DEV = 256
OWNERS = 128
BLOCKS = 256
N = 65536
CAP = 8
KPO = 8
PER = 1


def cluster_draw(key):
    base = jax.random.fold_in(key, 11)
    first_key, second_key, third_key, fourth_key = jax.random.split(base, 4)
    slots = OWNERS * CAP
    heat = jnp.argsort(jax.random.permutation(first_key, OWNERS)).astype(jnp.int32)
    places = jnp.arange(slots, dtype=jnp.int32)
    slot_owner = places // CAP
    slot_heat = heat[slot_owner]
    noise = jax.random.randint(second_key, (BLOCKS, slots), 0, 4096, dtype=jnp.int32)
    score = (1 + noise + slot_heat[None, :] * 512) * slots + places[None, :]
    score = jnp.where((slot_heat == 0)[None, :], places[None, :] + jnp.zeros_like(score), score)
    chosen = jnp.argsort(score, axis=1)[:, :ROW_DEV].astype(jnp.int32)
    shuffles = jax.vmap(lambda single: jax.random.permutation(single, ROW_DEV))(jax.random.split(third_key, BLOCKS))
    chosen = jnp.take_along_axis(chosen, shuffles.astype(jnp.int32), axis=1)
    owner = chosen // CAP
    shift = jax.random.randint(fourth_key, (BLOCKS, OWNERS), 0, KPO, dtype=jnp.int32)
    local = (chosen % CAP + jnp.take_along_axis(shift, owner, axis=1)) % KPO
    return (owner * KPO + local).reshape(N).astype(jnp.int32)


def draw_assignment(key, part):
    return cluster_draw(key)


def draw_embeddings(key, part):
    cluster = cluster_draw(key)
    centre_key, noise_key = jax.random.split(jax.random.fold_in(key, 23), 2)
    centres = jnp.clip(jax.random.normal(centre_key, (K, D), jnp.float32), -4.0, 4.0)
    noise = jnp.clip(jax.random.normal(noise_key, (N, D), jnp.float32), -4.0, 4.0)
    values = 0.8 * centres[cluster] + noise
    return values.astype(jnp.bfloat16)


def setup_inputs(seed: int = 0, part: int = 0) -> dict:
    arg_keys = jax.random.split(jax.random.key(seed), 4)
    own_keys = jax.random.split(jax.random.fold_in(arg_keys[3], part), 4)
    return {
        "embeddings": draw_embeddings(jax.random.fold_in(jax.random.fold_in(arg_keys[3], part), 71), part),
        "assignment": draw_assignment(jax.random.fold_in(jax.random.fold_in(arg_keys[3], part), 71), part),
        "order": jax.random.permutation(own_keys[2], N).astype(jnp.int32),
    }


EPSILON = 1e-06

def reference(embeddings, assignment, order):
    values = embeddings.astype(jnp.float32)
    unit_rows = (values * lax.rsqrt(lax.optimization_barrier(jnp.sum(values * values, axis=1, keepdims=True)) + EPSILON)).astype(jnp.bfloat16)
    members = jnp.argsort(assignment, stable=True).astype(jnp.int32)
    counts = jax.ops.segment_sum(jnp.ones((N,), jnp.int32), assignment, num_segments=K).astype(jnp.int32)
    starts = (jnp.cumsum(counts) - counts).astype(jnp.int32)
    window = BLOCKS * PER
    sorted_rows = jnp.concatenate([unit_rows[members], jnp.zeros((window, D), jnp.bfloat16)], axis=0)
    sorted_order = jnp.concatenate([order[members], jnp.zeros((window,), jnp.int32)], axis=0)

    def one_cluster(cluster):
        first = starts[cluster]
        total = counts[cluster]
        rows_here = lax.dynamic_slice_in_dim(sorted_rows, first, window, 0)
        order_here = lax.dynamic_slice_in_dim(sorted_order, first, window, 0)
        valid = jnp.arange(window, dtype=jnp.int32) < total
        gram = jnp.dot(rows_here, rows_here.T, preferred_element_type=jnp.float32)
        earlier = valid[None, :] & (order_here[None, :] < order_here[:, None])
        best_sim = jnp.maximum(lax.optimization_barrier(jnp.max(jnp.where(earlier, gram, -1.0), axis=1)), -1.0)
        floats = rows_here.astype(jnp.float32)
        centre = lax.optimization_barrier(jnp.sum(jnp.where(valid[:, None], floats, 0.0), axis=0)) / jnp.maximum(total, 1).astype(jnp.float32)
        offset = floats - centre[None, :]
        return (best_sim, lax.optimization_barrier(jnp.sum(offset * offset, axis=1)))
    best_all, dist_all = lax.map(one_cluster, jnp.arange(K, dtype=jnp.int32))
    position = jnp.argsort(members).astype(jnp.int32)
    within = (position - starts[assignment]).astype(jnp.int32)
    return (best_all[assignment, within], dist_all[assignment, within])
```

```python
import functools

import jax
import jax.numpy as jnp
from jax import lax
from jax.experimental import pallas as pl
from jax.experimental.pallas import tpu as pltpu
from jax.sharding import PartitionSpec as P

EPSILON = 1e-06
LANES = 128
CLUSTERS = 1024
SLOTS = 2
FIRST_OWNER_ROW = 3
MESH = pl.DeviceIdType.MESH
F32 = jnp.float32
BF16 = jnp.bfloat16


def iota(shape, dim):
    return lax.broadcasted_iota(jnp.int32, shape, dim)


def drain(ref, sem):
    pltpu.make_async_copy(ref, ref, sem).wait()


def kernel(
    sizes,
    emb_ref,
    cluster_ref,
    order_ref,
    base_ref,
    best_ref,
    dist_ref,
    used_ref,
    rank_ref,
    flags_out,
    flags_in,
    table_in,
    table_out,
    used_in,
    used_out,
    send_rows,
    send_order,
    got_rows,
    got_order,
    send_back,
    got_back,
    ready,
    flag_send,
    flag_recv,
    table_send,
    table_recv,
    used_send,
    used_recv,
    rows_send,
    rows_recv,
    order_send,
    order_recv,
    back_send,
    back_recv,
):
    nz, nx, nc, owner_rows, first_owner = sizes
    side = nx * nc
    blocks = nz * side
    owners = owner_rows * side
    count, width = emb_ref.shape
    pieces = width // LANES
    z = lax.axis_index("rows")
    x = lax.axis_index("sub")
    c = lax.axis_index("pair")
    xc = x * nc + c
    me = z * side + xc
    my_place = (z - first_owner) * side + xc
    is_owner = (z >= first_owner) & (z < first_owner + owner_rows)

    def device(tz, txc):
        return {"rows": tz, "sub": txc // nc, "pair": lax.rem(txc, nc)}

    def beside(k):
        return lax.rem(xc + k, side)

    def signal(sem, tz, txc):
        pl.semaphore_signal(sem, inc=1, device_id=device(tz, txc), device_id_type=MESH)

    def remote(src, dst, send, recv, tz, txc):
        return pltpu.make_async_remote_copy(
            src_ref=src,
            dst_ref=dst,
            send_sem=send,
            recv_sem=recv,
            device_id=device(tz, txc),
            device_id_type=MESH,
        )

    barrier = pltpu.get_barrier_semaphore()

    @pl.loop(1, side)
    def _(k):
        signal(barrier, z, beside(k))

    signal(barrier, lax.rem(z + 1, nz), xc)
    signal(barrier, lax.rem(z + nz - 1, nz), xc)

    cluster = cluster_ref[...]
    high = cluster // LANES
    low = cluster - high * LANES
    groups = CLUSTERS // LANES
    is_high = iota((groups, count), 0) == high
    is_low = (iota((LANES, count), 0) == low).astype(F32).astype(BF16)
    flags_out[...] = lax.dot_general(
        is_high.astype(F32).astype(BF16),
        is_low,
        (((1,), (1,)), ((), ())),
        preferred_element_type=F32,
    )

    pl.semaphore_wait(barrier, side - 1 + 2)

    @pl.loop(1, side)
    def _(k):
        remote(flags_out, flags_in.at[xc], flag_send, flag_recv, z, beside(k)).start()

    flags_in[xc] = flags_out[...]

    values = emb_ref[...].astype(F32)
    unit = (
        values * lax.rsqrt(jnp.sum(values * values, axis=1, keepdims=True) + EPSILON)
    ).astype(BF16)

    drain(flags_in.at[pl.ds(0, side - 1)], flag_recv)
    named = jnp.max(flags_in[...], axis=0)

    @pl.when(z == 0)
    def _():
        table_in[...] = jnp.zeros_like(table_in)

    upper = (iota((LANES, LANES), 0) < iota((LANES, LANES), 1)).astype(F32).astype(BF16)

    @pl.when(z > 0)
    def _():
        drain(table_in, table_recv)

    before = table_in[...]
    fresh = jnp.where((named > 0.0) & (before == 0.0), 1.0, 0.0)
    taken = jnp.max(before, axis=(0, 1), keepdims=True)
    inside = jnp.dot(fresh.astype(BF16), upper, preferred_element_type=F32)
    totals = jnp.sum(fresh, axis=1, keepdims=True)
    above = jnp.sum(
        jnp.where(
            iota((groups, groups), 0) > iota((groups, groups), 1),
            jnp.transpose(jnp.broadcast_to(totals, (groups, LANES)))[0:1, 0:groups],
            0.0,
        ),
        axis=1,
        keepdims=True,
    )
    table = jnp.where(fresh > 0.0, taken + above + inside + 1.0, before)
    table_out[...] = table

    @pl.when(z < nz - 1)
    def _():
        remote(table_out, table_in, table_send, table_recv, z + 1, xc).start()

    @pl.when(is_owner)
    def _():
        @pl.loop(0, z)
        def _(tz):
            signal(ready.at[z], tz, xc)

    used = jnp.broadcast_to(jnp.max(table, axis=(0, 1), keepdims=True), used_out.shape)
    used_out[...] = used

    @pl.when(z == nz - 1)
    def _():
        used_in[...] = used

        @pl.loop(0, nz - 1)
        def _(tz):
            remote(used_out, used_in, used_send, used_recv, tz, xc).start()

    tens = jnp.floor(table * (1.0 / 32.0))
    both = jnp.concatenate([tens, table - tens * 32.0], axis=0).astype(BF16)
    found = jnp.dot(both, is_low, preferred_element_type=F32)
    found = found[0:groups] * 32.0 + found[groups:]
    rank = jnp.sum(jnp.where(is_high, found, 0.0), axis=0, keepdims=True) - 1.0
    rank_ref[...] = rank
    slot = rank - base_ref[...]
    place = iota((owners, count), 0).astype(F32) * float(SLOTS)
    wanted = [place + float(s) == slot for s in range(SLOTS)]
    tiles = [
        jnp.dot(w.astype(F32).astype(BF16), unit, preferred_element_type=F32)
        for w in wanted
    ]
    send_rows[...] = (
        jnp.concatenate(tiles, axis=1)
        .reshape(owners, SLOTS * pieces, LANES)
        .astype(BF16)
    )
    position = order_ref[...].astype(F32) + 1.0
    orders = [
        jnp.sum(jnp.where(w, position, 0.0), axis=1, keepdims=True) for w in wanted
    ]
    lane = iota((owners, LANES), 1)
    send_order[...] = jnp.where(lane < LANES // 2, orders[0], orders[1]).reshape(
        owners, 1, LANES
    )

    def deliver(t, tz, txc):
        place = t * side + txc
        remote(
            send_order.at[place], got_order.at[me], order_send, order_recv, tz, txc
        ).start()
        remote(
            send_rows.at[place], got_rows.at[me], rows_send, rows_recv, tz, txc
        ).start()

    @pl.loop(0, owner_rows)
    def _(t):
        tz = t + first_owner

        @pl.when(tz > z)
        def _():
            pl.semaphore_wait(ready.at[tz], 1)

        @pl.loop(1, side)
        def _(k):
            deliver(t, tz, beside(k))

        @pl.when(tz != z)
        def _():
            deliver(t, tz, xc)

    @pl.when(is_owner)
    def _():
        got_rows[me] = send_rows[my_place]
        got_order[me] = send_order[my_place]
        drain(got_order.at[pl.ds(0, blocks - 1)], order_recv)
        drain(got_rows.at[pl.ds(0, blocks - 1)], rows_recv)
        members = got_rows[...].reshape(blocks, SLOTS * width)
        stamps = got_order[...].reshape(blocks, LANES)
        flipped = jnp.transpose(stamps)
        answers = []
        for s in range(SLOTS):
            rows = members[:, s * width : (s + 1) * width]
            at = s * (LANES // SLOTS)
            mine = stamps[:, at : at + 1]
            theirs = flipped[at : at + 1, :]
            gram = lax.dot_general(
                rows, rows, (((1,), (1,)), ((), ())), preferred_element_type=F32
            )
            earlier = (theirs > 0.0) & (theirs < mine)
            answers.append(
                jnp.max(jnp.where(earlier, gram, -1.0), axis=1, keepdims=True)
            )
            total = jnp.sum(
                jnp.where(theirs > 0.0, 1.0, 0.0), axis=1, keepdims=True
            )
            summed = jnp.dot(
                jnp.ones((8, blocks), BF16), rows, preferred_element_type=F32
            )[0:1]
            centre = summed / jnp.maximum(total, 1.0)
            offset = rows.astype(F32) - centre
            answers.append(jnp.sum(offset * offset, axis=1, keepdims=True))
        part = iota((blocks, LANES), 1) // (LANES // len(answers))
        answer = answers[-1]
        for n in range(len(answers) - 1):
            answer = jnp.where(part == n, answers[n], answer)
        send_back[...] = answer.reshape(blocks, 1, LANES)

        @pl.loop(0, nz)
        def _(tz):
            @pl.loop(1, side)
            def _(k):
                remote(
                    send_back.at[tz * side + beside(k)],
                    got_back.at[my_place],
                    back_send,
                    back_recv,
                    tz,
                    beside(k),
                ).start()

            @pl.when(tz != z)
            def _():
                remote(
                    send_back.at[tz * side + xc],
                    got_back.at[my_place],
                    back_send,
                    back_recv,
                    tz,
                    xc,
                ).start()

        got_back[my_place] = send_back[me]
        drain(got_back.at[pl.ds(0, owners - 1)], back_recv)

    @pl.when(jnp.logical_not(is_owner))
    def _():
        drain(got_back, back_recv)

    back = got_back[...].reshape(owners, LANES)
    step = LANES // (2 * SLOTS)
    best = jnp.zeros((1, count), F32)
    dist = jnp.zeros((1, count), F32)
    for s in range(SLOTS):
        at = 2 * s * step
        best += jnp.sum(
            jnp.where(wanted[s], back[:, at : at + 1], 0.0), axis=0, keepdims=True
        )
        dist += jnp.sum(
            jnp.where(wanted[s], back[:, at + step : at + step + 1], 0.0),
            axis=0,
            keepdims=True,
        )
    best_ref[...] = best
    dist_ref[...] = dist

    @pl.when(z < nz - 1)
    def _():
        drain(used_in, used_recv)
        drain(table_out, table_send)

    @pl.when(z == nz - 1)
    def _():
        @pl.loop(0, nz - 1)
        def _(tz):
            drain(used_out, used_send)

    used_ref[...] = used_in[...]
    drain(flags_in.at[pl.ds(0, side - 1)], flag_send)

    @pl.when(is_owner)
    def _():
        drain(send_rows.at[pl.ds(0, owners - 1)], rows_send)
        drain(send_order.at[pl.ds(0, owners - 1)], order_send)
        drain(send_back.at[pl.ds(0, blocks - 1)], back_send)

    @pl.when(jnp.logical_not(is_owner))
    def _():
        drain(send_rows, rows_send)
        drain(send_order, order_send)


def one_round(sizes, embeddings, cluster, order, base):
    nz, nx, nc, owner_rows, _ = sizes
    side = nx * nc
    blocks = nz * side
    owners = owner_rows * side
    count, width = embeddings.shape
    tiles = SLOTS * width // LANES
    groups = CLUSTERS // LANES
    vmem = pl.BlockSpec(memory_space=pltpu.VMEM)
    row = jax.ShapeDtypeStruct((1, count), F32)
    dma = pltpu.SemaphoreType.DMA
    return pl.pallas_call(
        functools.partial(kernel, sizes),
        out_shape=(row, row, jax.ShapeDtypeStruct((1, LANES), F32), row),
        in_specs=[vmem] * 4,
        out_specs=(vmem,) * 4,
        scratch_shapes=[
            pltpu.VMEM((groups, LANES), F32),
            pltpu.VMEM((side, groups, LANES), F32),
            pltpu.VMEM((groups, LANES), F32),
            pltpu.VMEM((groups, LANES), F32),
            pltpu.VMEM((1, LANES), F32),
            pltpu.VMEM((1, LANES), F32),
            pltpu.VMEM((owners, tiles, LANES), BF16),
            pltpu.VMEM((owners, 1, LANES), F32),
            pltpu.VMEM((blocks, tiles, LANES), BF16),
            pltpu.VMEM((blocks, 1, LANES), F32),
            pltpu.VMEM((blocks, 1, LANES), F32),
            pltpu.VMEM((owners, 1, LANES), F32),
            pltpu.SemaphoreType.REGULAR((nz,)),
        ]
        + [dma] * 12,
        compiler_params=pltpu.CompilerParams(collective_id=0, has_side_effects=True),
    )(embeddings, cluster, order, base)


def per_device(embeddings, assignment, order):
    nz, nx, nc = (lax.axis_size(a) for a in ("rows", "sub", "pair"))
    count = embeddings.shape[0]
    capacity = count + count // 4
    owner_rows = capacity // (SLOTS * nx * nc)
    capacity = owner_rows * SLOTS * nx * nc
    sizes = (nz, nx, nc, owner_rows, FIRST_OWNER_ROW)
    run = functools.partial(
        one_round,
        sizes,
        embeddings,
        assignment.reshape(1, count),
        order.reshape(1, count),
    )
    best, dist, used, _ = run(jnp.zeros((1, count), F32))

    def unfinished(state):
        return state[2] < used[0, 0]

    def next_round(state):
        best, dist, base = state
        more_best, more_dist, _, rank = run(jnp.full((1, count), base))
        late = (rank >= base) & (rank < base + capacity)
        return (
            jnp.where(late, more_best, best),
            jnp.where(late, more_dist, dist),
            base + capacity,
        )

    best, dist, _ = lax.while_loop(
        unfinished, next_round, (best, dist, jnp.float32(capacity))
    )
    return best.reshape(count), dist.reshape(count)


def solution(mesh):
    in_specs = (
        P(("groups", "rows", "sub", "pair"), None),
        P(("groups", "rows", "sub", "pair")),
        P(("groups", "rows", "sub", "pair")),
    )
    out_specs = (P(("groups", "rows", "sub", "pair")), P(("groups", "rows", "sub", "pair")))
    return jax.shard_map(
        per_device, mesh=mesh, in_specs=in_specs, out_specs=out_specs, check_vma=False
    )
```

```python
import functools

import jax
import jax.numpy as jnp
from jax import lax
from jax.experimental import pallas as pl
from jax.experimental.pallas import tpu as pltpu
from jax.sharding import PartitionSpec as P

EPSILON = 1e-06
LANES = 128
CLUSTERS = 1024
SLOTS = 2
MESH = pl.DeviceIdType.MESH
F32 = jnp.float32
BF16 = jnp.bfloat16


def iota(shape, dim):
    return lax.broadcasted_iota(jnp.int32, shape, dim)


def padded(rows):
    return -(-rows // 8) * 8


def drain(ref, sem):
    pltpu.make_async_copy(ref, ref, sem).wait()


def kernel(
    sizes,
    emb_ref,
    cluster_ref,
    order_ref,
    base_ref,
    best_ref,
    dist_ref,
    used_ref,
    rank_ref,
    flags_out,
    flags_in,
    named,
    used_in,
    used_out,
    send_rows,
    order_out,
    order_mid,
    send_order,
    got_rows,
    got_order,
    answers,
    gathered,
    send_back,
    got_back,
    ready,
    next_in,
    named_recv,
    flag_send,
    flag_recv,
    named_send,
    used_send,
    used_recv,
    rows_send,
    rows_recv,
    mid_send,
    mid_recv,
    order_send,
    order_recv,
    answer_send,
    answer_recv,
    back_send,
    back_recv,
):
    nz, nx, nc, owner_rows = sizes
    side = nx * nc
    blocks = nz * side
    owners = owner_rows * side
    share = LANES // side
    pad = padded(owner_rows)
    count, width = emb_ref.shape
    pieces = width // LANES
    z = lax.rem(lax.axis_index("rows") + nz - 1, nz)
    x = lax.axis_index("sub")
    c = lax.axis_index("pair")
    xc = x * nc + c
    me = xc * nz + z
    owner_row = (z * owner_rows + nz - 1) // nz
    is_owner = (owner_row * nz) // owner_rows == z
    my_place = owner_row * side + xc

    def device(tz, txc):
        return {
            "rows": lax.rem(tz + 1, nz),
            "sub": txc // nc,
            "pair": lax.rem(txc, nc),
        }

    def beside(k):
        return lax.rem(xc + k, side)

    def signal(sem, tz, txc):
        pl.semaphore_signal(sem, inc=1, device_id=device(tz, txc), device_id_type=MESH)

    def remote(src, dst, send, recv, tz, txc):
        return pltpu.make_async_remote_copy(
            src_ref=src,
            dst_ref=dst,
            send_sem=send,
            recv_sem=recv,
            device_id=device(tz, txc),
            device_id_type=MESH,
        )

    barrier = pltpu.get_barrier_semaphore()

    @pl.loop(1, side)
    def _(k):
        signal(barrier, z, beside(k))

    @pl.when(z < nz - 1)
    def _():
        signal(barrier, z + 1, xc)

    cluster = cluster_ref[...]
    high = cluster // LANES
    low = cluster - high * LANES
    groups = CLUSTERS // LANES
    is_high = iota((groups, count), 0) == high
    is_low = (iota((LANES, count), 0) == low).astype(F32).astype(BF16)
    flags_out[...] = lax.dot_general(
        is_high.astype(F32).astype(BF16),
        is_low,
        (((1,), (1,)), ((), ())),
        preferred_element_type=F32,
    )

    pl.semaphore_wait(barrier, side - 1 + (z + nz - 1) // nz)

    @pl.when(z > 0)
    def _():
        signal(next_in, z - 1, xc)

    @pl.loop(1, side)
    def _(k):
        remote(flags_out, flags_in.at[xc], flag_send, flag_recv, z, beside(k)).start()

    flags_in[xc] = flags_out[...]

    values = emb_ref[...].astype(F32)
    unit = (
        values * lax.rsqrt(jnp.sum(values * values, axis=1, keepdims=True) + EPSILON)
    ).astype(BF16)

    drain(flags_in.at[pl.ds(0, side - 1)], flag_recv)
    named[z] = jnp.max(flags_in[...], axis=0)

    def pass_on(tz):
        @pl.when(z < nz - 1)
        def _():
            remote(
                named.at[tz], named.at[tz], named_send, named_recv.at[tz], z + 1, xc
            ).start()

    @pl.when(z < nz - 1)
    def _():
        pl.semaphore_wait(next_in, 1)

    @pl.loop(0, z)
    def _(tz):
        drain(named.at[tz], named_recv.at[tz])
        pass_on(tz)

        @pl.when(is_owner)
        def _():
            signal(ready.at[z], tz, xc)

    pass_on(z)

    seen = jnp.zeros((groups, LANES), F32)
    fresh = []
    for tz in range(nz):
        here = jnp.where(z >= tz, named[tz], 0.0)
        fresh.append(jnp.where((here > 0.0) & (seen == 0.0), 1.0, 0.0))
        seen = jnp.maximum(seen, here)
    firsts = jnp.concatenate(fresh, axis=0).astype(BF16)
    levels = nz * groups
    upper = (iota((LANES, LANES), 0) < iota((LANES, LANES), 1)).astype(F32).astype(BF16)
    lower = (iota((levels, levels), 0) > iota((levels, levels), 1)).astype(F32)
    inside = jnp.dot(firsts, upper, preferred_element_type=F32)
    above = jnp.sum(
        jnp.dot(lower.astype(BF16), firsts, preferred_element_type=F32),
        axis=1,
        keepdims=True,
    )
    ranks = inside + above + 1.0
    table = jnp.zeros((groups, LANES), F32)
    for tz in range(nz):
        table += fresh[tz] * ranks[tz * groups : (tz + 1) * groups]

    used = jnp.broadcast_to(jnp.max(table, axis=(0, 1), keepdims=True), used_out.shape)
    used_out[...] = used

    @pl.when(z == nz - 1)
    def _():
        used_in[...] = used

        @pl.loop(0, nz - 1)
        def _(tz):
            remote(used_out, used_in, used_send, used_recv, tz, xc).start()

    tens = jnp.floor(table * (1.0 / 32.0))
    both = jnp.concatenate([tens, table - tens * 32.0], axis=0).astype(BF16)
    found = jnp.dot(both, is_low, preferred_element_type=F32)
    found = found[0:groups] * 32.0 + found[groups:]
    rank = jnp.sum(jnp.where(is_high, found, 0.0), axis=0, keepdims=True) - 1.0
    rank_ref[...] = rank
    slot = rank if base_ref is None else rank - base_ref[...]
    place = iota((owners, count), 0).astype(F32) * float(SLOTS)
    wanted = [place + float(s) == slot for s in range(SLOTS)]
    tiles = [
        jnp.dot(w.astype(F32).astype(BF16), unit, preferred_element_type=F32)
        for w in wanted
    ]
    send_rows[...] = (
        jnp.concatenate(tiles, axis=1)
        .reshape(owners, SLOTS * pieces, LANES)
        .astype(BF16)
    )
    position = order_ref[...].astype(F32) + 1.0
    line = iota((side * pad, count), 0)
    at_row = lax.rem(line, pad)
    place = jnp.where(at_row < owner_rows, at_row * side + line // pad, -CLUSTERS)
    place = place.astype(F32) * float(SLOTS)
    orders = [
        jnp.sum(
            jnp.where(place + float(s) == slot, position, 0.0), axis=1, keepdims=True
        )
        for s in range(SLOTS)
    ]
    even = lax.rem(iota((side * pad, LANES), 1), SLOTS) == 0
    order_out[...] = jnp.where(even, orders[0], orders[1])

    @pl.loop(1, side, unroll=3)
    def _(k):
        remote(
            order_out.at[pl.ds(pl.multiple_of(beside(k) * pad, pad), pad)],
            order_mid.at[xc],
            mid_send,
            mid_recv,
            z,
            beside(k),
        ).start()

    order_mid[xc] = order_out[pl.ds(pl.multiple_of(xc * pad, pad), pad), :]

    def deliver(t, tz, txc):
        place = t * side + txc
        remote(
            send_rows.at[place], got_rows.at[me], rows_send, rows_recv, tz, txc
        ).start()

    @pl.loop(0, owner_rows)
    def _(t):
        tz = (t * nz) // owner_rows

        @pl.when(tz > z)
        def _():
            pl.semaphore_wait(ready.at[tz], 1)

        @pl.loop(1, side, unroll=5)
        def _(k):
            deliver(t, tz, beside(k))

        @pl.when(tz != z)
        def _():
            deliver(t, tz, xc)

    drain(order_mid.at[pl.ds(0, side - 1)], mid_recv)
    origin = iota((pad, LANES), 1) // share
    packed = order_mid[side - 1]
    for n in range(side - 1):
        packed = jnp.where(origin == n, order_mid[n], packed)
    send_order[...] = packed.reshape(pad, 1, LANES)

    @pl.loop(0, owner_rows)
    def _(t):
        tz = (t * nz) // owner_rows

        @pl.when(tz != z)
        def _():
            remote(
                send_order.at[t], got_order.at[z], order_send, order_recv, tz, xc
            ).start()

    @pl.when(is_owner)
    def _():
        got_rows[me] = send_rows[my_place]
        got_order[z] = send_order[owner_row]
        drain(got_order.at[pl.ds(0, nz - 1)], order_recv)
        drain(got_rows.at[pl.ds(0, blocks - 1)], rows_recv)
        members = got_rows[...].reshape(blocks, SLOTS * width)
        arrived = got_order[...].reshape(nz, LANES)
        spread = [
            jnp.concatenate(
                [
                    jnp.broadcast_to(
                        arrived[:, n * share + s : n * share + s + 1], (nz, LANES)
                    )
                    for n in range(side)
                ],
                axis=0,
            )
            for s in range(SLOTS)
        ]
        half = iota((blocks, LANES), 1) < LANES // SLOTS
        stamps = jnp.where(half, spread[0], spread[1])
        flipped = jnp.transpose(stamps)
        values = []
        for s in range(SLOTS):
            rows = members[:, s * width : (s + 1) * width]
            at = s * (LANES // SLOTS)
            mine = stamps[:, at : at + 1]
            theirs = flipped[at : at + 1, :]
            gram = lax.dot_general(
                rows, rows, (((1,), (1,)), ((), ())), preferred_element_type=F32
            )
            earlier = (theirs > 0.0) & (theirs < mine)
            values.append(
                jnp.max(jnp.where(earlier, gram, -1.0), axis=1, keepdims=True)
            )
            total = jnp.sum(
                jnp.where(theirs > 0.0, 1.0, 0.0), axis=1, keepdims=True
            )
            summed = jnp.dot(
                jnp.ones((8, blocks), BF16), rows, preferred_element_type=F32
            )[0:1]
            centre = summed / jnp.maximum(total, 1.0)
            offset = rows.astype(F32) - centre
            values.append(jnp.sum(offset * offset, axis=1, keepdims=True))
        kind = lax.rem(iota((blocks, LANES), 1), len(values))
        answer = values[-1]
        for n in range(len(values) - 1):
            answer = jnp.where(kind == n, values[n], answer)
        answers[...] = answer

        @pl.loop(1, side)
        def _(k):
            remote(
                answers.at[pl.ds(pl.multiple_of(beside(k) * nz, nz), nz)],
                gathered.at[xc],
                answer_send,
                answer_recv,
                z,
                beside(k),
            ).start()

        gathered[xc] = answers[pl.ds(pl.multiple_of(xc * nz, nz), nz), :]
        drain(gathered.at[pl.ds(0, side - 1)], answer_recv)
        source = iota((nz, LANES), 1) // share
        packed = gathered[side - 1]
        for n in range(side - 1):
            packed = jnp.where(source == n, gathered[n], packed)
        send_back[...] = packed.reshape(nz, 1, LANES)

        @pl.loop(0, nz)
        def _(tz):
            @pl.when(tz != z)
            def _():
                remote(
                    send_back.at[tz],
                    got_back.at[owner_row],
                    back_send,
                    back_recv,
                    tz,
                    xc,
                ).start()

        got_back[owner_row] = send_back[z]
        drain(got_back.at[pl.ds(0, owner_rows - 1)], back_recv)

    @pl.when(jnp.logical_not(is_owner))
    def _():
        drain(got_back, back_recv)

    back = got_back[...].reshape(owner_rows, LANES)
    columns = jnp.transpose(
        jnp.concatenate(
            [back, jnp.zeros((LANES - owner_rows, LANES), F32)], axis=0
        )
    )
    owner = jnp.floor(slot * (1.0 / SLOTS))
    at_row = jnp.floor(owner * (1.0 / side))
    at_lane = (owner - at_row * side) * share + (slot - owner * SLOTS) * 2.0
    picked = jnp.zeros((LANES, count), F32)
    for t in range(owner_rows):
        picked = jnp.where(at_row == float(t), columns[:, t : t + 1], picked)
    lane = iota((LANES, count), 0).astype(F32)
    best_ref[...] = jnp.sum(
        jnp.where(lane == at_lane, picked, 0.0), axis=0, keepdims=True
    )
    dist_ref[...] = jnp.sum(
        jnp.where(lane == at_lane + 1.0, picked, 0.0), axis=0, keepdims=True
    )

    @pl.when(z < nz - 1)
    def _():
        drain(used_in, used_recv)

        @pl.loop(0, z + 1)
        def _(tz):
            drain(named.at[tz], named_send)

    @pl.when(z == nz - 1)
    def _():
        @pl.loop(0, nz - 1)
        def _(tz):
            drain(used_out, used_send)

    used_ref[...] = used_in[...]
    drain(flags_in.at[pl.ds(0, side - 1)], flag_send)
    drain(order_mid.at[pl.ds(0, side - 1)], mid_send)

    @pl.when(is_owner)
    def _():
        drain(send_rows.at[pl.ds(0, owners - 1)], rows_send)
        drain(send_order.at[pl.ds(0, owner_rows - 1)], order_send)
        drain(gathered.at[pl.ds(0, side - 1)], answer_send)
        drain(send_back.at[pl.ds(0, nz - 1)], back_send)

    @pl.when(jnp.logical_not(is_owner))
    def _():
        drain(send_rows, rows_send)
        drain(send_order.at[pl.ds(0, owner_rows)], order_send)


def one_round(sizes, embeddings, cluster, order, base):
    nz, nx, nc, owner_rows = sizes
    side = nx * nc
    blocks = nz * side
    owners = owner_rows * side
    count, width = embeddings.shape
    tiles = SLOTS * width // LANES
    groups = CLUSTERS // LANES
    vmem = pl.BlockSpec(memory_space=pltpu.VMEM)
    row = jax.ShapeDtypeStruct((1, count), F32)
    dma = pltpu.SemaphoreType.DMA
    inputs = (embeddings, cluster, order)
    if base is None:

        def body(emb_ref, cluster_ref, order_ref, *refs):
            kernel(sizes, emb_ref, cluster_ref, order_ref, None, *refs)

    else:
        inputs += (base,)
        body = functools.partial(kernel, sizes)
    return pl.pallas_call(
        body,
        out_shape=(row, row, jax.ShapeDtypeStruct((1, LANES), F32), row),
        in_specs=[vmem] * len(inputs),
        out_specs=(vmem,) * 4,
        scratch_shapes=[
            pltpu.VMEM((groups, LANES), F32),
            pltpu.VMEM((side, groups, LANES), F32),
            pltpu.VMEM((nz, groups, LANES), F32),
            pltpu.VMEM((1, LANES), F32),
            pltpu.VMEM((1, LANES), F32),
            pltpu.VMEM((owners, tiles, LANES), BF16),
            pltpu.VMEM((side * padded(owner_rows), LANES), F32),
            pltpu.VMEM((side, padded(owner_rows), LANES), F32),
            pltpu.VMEM((padded(owner_rows), 1, LANES), F32),
            pltpu.VMEM((blocks, tiles, LANES), BF16),
            pltpu.VMEM((nz, 1, LANES), F32),
            pltpu.VMEM((blocks, LANES), F32),
            pltpu.VMEM((side, nz, LANES), F32),
            pltpu.VMEM((nz, 1, LANES), F32),
            pltpu.VMEM((owner_rows, 1, LANES), F32),
            pltpu.SemaphoreType.REGULAR((nz,)),
            pltpu.SemaphoreType.REGULAR,
            dma((nz,)),
        ]
        + [dma] * 15,
        compiler_params=pltpu.CompilerParams(
            collective_id=0 if base is None else 1, has_side_effects=True
        ),
    )(*inputs)


def per_device(embeddings, assignment, order):
    nz, nx, nc = (lax.axis_size(a) for a in ("rows", "sub", "pair"))
    count = embeddings.shape[0]
    capacity = count + count // 4
    owner_rows = capacity // (SLOTS * nx * nc)
    capacity = owner_rows * SLOTS * nx * nc
    sizes = (nz, nx, nc, owner_rows)
    run = functools.partial(
        one_round,
        sizes,
        embeddings,
        assignment.reshape(1, count),
        order.reshape(1, count),
    )
    best, dist, used, _ = run(None)

    def unfinished(state):
        return state[2] < used[0, 0]

    def next_round(state):
        best, dist, base = state
        more_best, more_dist, _, rank = run(jnp.full((1, count), base))
        late = (rank >= base) & (rank < base + capacity)
        return (
            jnp.where(late, more_best, best),
            jnp.where(late, more_dist, dist),
            base + capacity,
        )

    best, dist, _ = lax.while_loop(
        unfinished, next_round, (best, dist, jnp.float32(capacity))
    )
    return best.reshape(count), dist.reshape(count)


def solution(mesh):
    in_specs = (
        P(("groups", "rows", "sub", "pair"), None),
        P(("groups", "rows", "sub", "pair")),
        P(("groups", "rows", "sub", "pair")),
    )
    out_specs = (P(("groups", "rows", "sub", "pair")), P(("groups", "rows", "sub", "pair")))
    return jax.shard_map(
        per_device, mesh=mesh, in_specs=in_specs, out_specs=out_specs, check_vma=False
    )
```

```python
import functools

import jax
import jax.numpy as jnp
from jax import lax
from jax.experimental import pallas as pl
from jax.experimental.pallas import tpu as pltpu
from jax.sharding import PartitionSpec as P

EPSILON = 1e-06
LANES = 128
CLUSTERS = 1024
SLOTS = 2
SPARSE = 4
MESH = pl.DeviceIdType.MESH
F32 = jnp.float32
BF16 = jnp.bfloat16


def iota(shape, dim):
    return lax.broadcasted_iota(jnp.int32, shape, dim)


def drain(ref, sem):
    pltpu.make_async_copy(ref, ref, sem).wait()


def kernel(
    sizes,
    emb_ref,
    cluster_ref,
    order_ref,
    base_ref,
    best_ref,
    dist_ref,
    used_ref,
    rank_ref,
    flags_out,
    flags_in,
    named,
    used_in,
    used_out,
    send_rows,
    send_doubles,
    order_out,
    order_mid,
    send_order,
    got_rows,
    got_doubles,
    got_order,
    answers,
    gathered,
    send_back,
    got_back,
    ready,
    next_in,
    named_recv,
    flag_send,
    flag_recv,
    named_send,
    used_send,
    used_recv,
    rows_send,
    rows_recv,
    doubles_send,
    doubles_recv,
    mid_send,
    mid_recv,
    order_send,
    order_recv,
    answer_send,
    answer_recv,
    back_send,
    back_recv,
):
    nz, nx, nc = sizes
    side = nx * nc
    blocks = nz * side
    doubles = side // SPARSE
    share = LANES // side
    count, width = emb_ref.shape
    pieces = width // LANES
    z = lax.rem(lax.axis_index("rows") + nz - 1, nz)
    x = lax.axis_index("sub")
    c = lax.axis_index("pair")
    xc = x * nc + c
    me = xc * nz + z
    my_place = z * side + xc
    my_double = z * doubles + xc // SPARSE
    is_double = lax.rem(xc, SPARSE) == 0

    def device(tz, txc):
        return {
            "rows": lax.rem(tz + 1, nz),
            "sub": txc // nc,
            "pair": lax.rem(txc, nc),
        }

    def beside(k):
        return lax.rem(xc + k, side)

    def signal(sem, tz, txc):
        pl.semaphore_signal(sem, inc=1, device_id=device(tz, txc), device_id_type=MESH)

    def remote(src, dst, send, recv, tz, txc):
        return pltpu.make_async_remote_copy(
            src_ref=src,
            dst_ref=dst,
            send_sem=send,
            recv_sem=recv,
            device_id=device(tz, txc),
            device_id_type=MESH,
        )

    barrier = pltpu.get_barrier_semaphore()

    @pl.loop(1, side)
    def _(k):
        signal(barrier, z, beside(k))

    @pl.when(z < nz - 1)
    def _():
        signal(barrier, z + 1, xc)

    cluster = cluster_ref[...]
    high = cluster // LANES
    low = cluster - high * LANES
    groups = CLUSTERS // LANES
    is_high = iota((groups, count), 0) == high
    is_low = (iota((LANES, count), 0) == low).astype(F32).astype(BF16)
    flags_out[...] = lax.dot_general(
        is_high.astype(F32).astype(BF16),
        is_low,
        (((1,), (1,)), ((), ())),
        preferred_element_type=F32,
    )

    pl.semaphore_wait(barrier, side - 1 + (z + nz - 1) // nz)

    @pl.when(z > 0)
    def _():
        signal(next_in, z - 1, xc)

    @pl.loop(1, side)
    def _(k):
        remote(flags_out, flags_in.at[xc], flag_send, flag_recv, z, beside(k)).start()

    flags_in[xc] = flags_out[...]

    values = emb_ref[...].astype(F32)
    unit = (
        values * lax.rsqrt(jnp.sum(values * values, axis=1, keepdims=True) + EPSILON)
    ).astype(BF16)

    drain(flags_in.at[pl.ds(0, side - 1)], flag_recv)
    named[z] = jnp.max(flags_in[...], axis=0)

    def pass_on(tz):
        @pl.when(z < nz - 1)
        def _():
            remote(
                named.at[tz], named.at[tz], named_send, named_recv.at[tz], z + 1, xc
            ).start()

    @pl.when(z < nz - 1)
    def _():
        pl.semaphore_wait(next_in, 1)

    @pl.loop(0, z)
    def _(tz):
        drain(named.at[tz], named_recv.at[tz])
        pass_on(tz)
        signal(ready.at[z], tz, xc)

    pass_on(z)

    seen = jnp.zeros((groups, LANES), F32)
    fresh = []
    for tz in range(nz):
        here = jnp.where(z >= tz, named[tz], 0.0)
        fresh.append(jnp.where((here > 0.0) & (seen == 0.0), 1.0, 0.0))
        seen = jnp.maximum(seen, here)
    firsts = jnp.concatenate(fresh, axis=0).astype(BF16)
    levels = nz * groups
    upper = (iota((LANES, LANES), 0) < iota((LANES, LANES), 1)).astype(F32).astype(BF16)
    lower = (iota((levels, levels), 0) > iota((levels, levels), 1)).astype(F32)
    inside = jnp.dot(firsts, upper, preferred_element_type=F32)
    above = jnp.sum(
        jnp.dot(lower.astype(BF16), firsts, preferred_element_type=F32),
        axis=1,
        keepdims=True,
    )
    ranks = inside + above + 1.0
    table = jnp.zeros((groups, LANES), F32)
    for tz in range(nz):
        table += fresh[tz] * ranks[tz * groups : (tz + 1) * groups]

    used = jnp.broadcast_to(jnp.max(table, axis=(0, 1), keepdims=True), used_out.shape)
    used_out[...] = used

    @pl.when(z == nz - 1)
    def _():
        used_in[...] = used

        @pl.loop(0, nz - 1)
        def _(tz):
            remote(used_out, used_in, used_send, used_recv, tz, xc).start()

    tens = jnp.floor(table * (1.0 / 32.0))
    both = jnp.concatenate([tens, table - tens * 32.0], axis=0).astype(BF16)
    found = jnp.dot(both, is_low, preferred_element_type=F32)
    found = found[0:groups] * 32.0 + found[groups:]
    rank = jnp.sum(jnp.where(is_high, found, 0.0), axis=0, keepdims=True) - 1.0
    rank_ref[...] = rank
    slot = rank if base_ref is None else rank - base_ref[...]
    wanted = [
        iota((blocks, count), 0).astype(F32) == slot,
        iota((nz * doubles, count), 0).astype(F32) + float(blocks) == slot,
    ]
    for w, send in zip(wanted, (send_rows, send_doubles)):
        tiles = jnp.dot(w.astype(F32).astype(BF16), unit, preferred_element_type=F32)
        send[...] = tiles.reshape(w.shape[0], pieces, LANES).astype(BF16)
    position = order_ref[...].astype(F32) + 1.0
    line = iota((blocks, count), 0)
    at_row = lax.rem(line, nz)
    column = line // nz
    places = [
        at_row * side + column,
        jnp.where(
            lax.rem(column, SPARSE) == 0,
            blocks + at_row * doubles + column // SPARSE,
            -CLUSTERS,
        ),
    ]
    orders = [
        jnp.sum(jnp.where(p.astype(F32) == slot, position, 0.0), axis=1, keepdims=True)
        for p in places
    ]
    even = lax.rem(iota((blocks, LANES), 1), SLOTS) == 0
    order_out[...] = jnp.where(even, orders[0], orders[1])

    @pl.loop(1, side, unroll=3)
    def _(k):
        remote(
            order_out.at[pl.ds(pl.multiple_of(beside(k) * nz, nz), nz)],
            order_mid.at[xc],
            mid_send,
            mid_recv,
            z,
            beside(k),
        ).start()

    order_mid[xc] = order_out[pl.ds(pl.multiple_of(xc * nz, nz), nz), :]

    def deliver(tz, txc):
        remote(
            send_rows.at[tz * side + txc], got_rows.at[me], rows_send, rows_recv, tz, txc
        ).start()

    def deliver_double(tz, q):
        remote(
            send_doubles.at[tz * doubles + q],
            got_doubles.at[me],
            doubles_send,
            doubles_recv,
            tz,
            q * SPARSE,
        ).start()

    @pl.loop(0, nz)
    def _(tz):
        @pl.when(tz > z)
        def _():
            pl.semaphore_wait(ready.at[tz], 1)

        @pl.loop(1, side, unroll=5)
        def _(k):
            deliver(tz, beside(k))

        @pl.when(tz != z)
        def _():
            deliver(tz, xc)

            @pl.loop(0, doubles)
            def _(q):
                deliver_double(tz, q)

        @pl.when(tz == z)
        def _():
            @pl.loop(0, doubles)
            def _(q):
                @pl.when(q * SPARSE != xc)
                def _():
                    deliver_double(tz, q)

    drain(order_mid.at[pl.ds(0, side - 1)], mid_recv)
    origin = iota((nz, LANES), 1) // share
    packed = order_mid[side - 1]
    for n in range(side - 1):
        packed = jnp.where(origin == n, order_mid[n], packed)
    send_order[...] = packed.reshape(nz, 1, LANES)

    @pl.loop(0, nz)
    def _(tz):
        @pl.when(tz != z)
        def _():
            remote(
                send_order.at[tz], got_order.at[z], order_send, order_recv, tz, xc
            ).start()

    got_rows[me] = send_rows[my_place]
    got_order[z] = send_order[z]
    drain(got_order.at[pl.ds(0, nz - 1)], order_recv)
    arrived = got_order[...].reshape(nz, LANES)
    kind = lax.rem(iota((blocks, LANES), 1), 2 * SLOTS)

    def judge(s, got):
        rows = got[...].reshape(blocks, width)
        stamps = jnp.concatenate(
            [
                jnp.broadcast_to(
                    arrived[:, n * share + s : n * share + s + 1], (nz, LANES)
                )
                for n in range(side)
            ],
            axis=0,
        )
        mine = stamps[:, 0:1]
        theirs = jnp.transpose(stamps)[0:1, :]
        gram = lax.dot_general(
            rows, rows, (((1,), (1,)), ((), ())), preferred_element_type=F32
        )
        earlier = (theirs > 0.0) & (theirs < mine)
        nearest = jnp.max(jnp.where(earlier, gram, -1.0), axis=1, keepdims=True)
        total = jnp.sum(jnp.where(theirs > 0.0, 1.0, 0.0), axis=1, keepdims=True)
        summed = jnp.dot(
            jnp.ones((8, blocks), BF16), rows, preferred_element_type=F32
        )[0:1]
        offset = rows.astype(F32) - summed / jnp.maximum(total, 1.0)
        apart = jnp.sum(offset * offset, axis=1, keepdims=True)
        return nearest, apart

    drain(got_rows.at[pl.ds(0, blocks - 1)], rows_recv)
    nearest, apart = judge(0, got_rows)
    answers[...] = jnp.where(kind == 0, nearest, apart)

    @pl.when(is_double)
    def _():
        got_doubles[me] = send_doubles[my_double]
        drain(got_doubles.at[pl.ds(0, blocks - 1)], doubles_recv)
        nearest, apart = judge(1, got_doubles)
        answers[...] = jnp.where(
            kind == 2, nearest, jnp.where(kind == 3, apart, answers[...])
        )

    @pl.loop(1, side, unroll=3)
    def _(k):
        remote(
            answers.at[pl.ds(pl.multiple_of(beside(k) * nz, nz), nz)],
            gathered.at[xc],
            answer_send,
            answer_recv,
            z,
            beside(k),
        ).start()

    gathered[xc] = answers[pl.ds(pl.multiple_of(xc * nz, nz), nz), :]
    drain(gathered.at[pl.ds(0, side - 1)], answer_recv)
    source = iota((nz, LANES), 1) // share
    packed = gathered[side - 1]
    for n in range(side - 1):
        packed = jnp.where(source == n, gathered[n], packed)
    send_back[...] = packed.reshape(nz, 1, LANES)

    @pl.loop(0, nz)
    def _(tz):
        @pl.when(tz != z)
        def _():
            remote(
                send_back.at[tz], got_back.at[z], back_send, back_recv, tz, xc
            ).start()

    got_back[z] = send_back[z]
    drain(got_back.at[pl.ds(0, nz - 1)], back_recv)

    back = got_back[...].reshape(nz, LANES)
    columns = jnp.transpose(
        jnp.concatenate([back, jnp.zeros((LANES - nz, LANES), F32)], axis=0)
    )
    double = slot >= float(blocks)
    per_row = jnp.where(double, float(doubles), float(side))
    index = jnp.where(double, slot - float(blocks), slot)
    at_row = jnp.floor(index / per_row)
    step = jnp.where(double, float(SPARSE * share), float(share))
    at_lane = (index - at_row * per_row) * step + jnp.where(double, 2.0, 0.0)
    picked = jnp.zeros((LANES, count), F32)
    for t in range(nz):
        picked = jnp.where(at_row == float(t), columns[:, t : t + 1], picked)
    lane = iota((LANES, count), 0).astype(F32)
    best_ref[...] = jnp.sum(
        jnp.where(lane == at_lane, picked, 0.0), axis=0, keepdims=True
    )
    dist_ref[...] = jnp.sum(
        jnp.where(lane == at_lane + 1.0, picked, 0.0), axis=0, keepdims=True
    )

    @pl.when(z < nz - 1)
    def _():
        drain(used_in, used_recv)

        @pl.loop(0, z + 1)
        def _(tz):
            drain(named.at[tz], named_send)

    @pl.when(z == nz - 1)
    def _():
        @pl.loop(0, nz - 1)
        def _(tz):
            drain(used_out, used_send)

    used_ref[...] = used_in[...]
    drain(flags_in.at[pl.ds(0, side - 1)], flag_send)
    drain(order_mid.at[pl.ds(0, side - 1)], mid_send)
    drain(gathered.at[pl.ds(0, side - 1)], answer_send)
    drain(send_order.at[pl.ds(0, nz - 1)], order_send)
    drain(send_back.at[pl.ds(0, nz - 1)], back_send)
    drain(send_rows.at[pl.ds(0, blocks - 1)], rows_send)
    drain(send_doubles.at[pl.ds(0, nz * doubles - 1)], doubles_send)

    @pl.when(jnp.logical_not(is_double))
    def _():
        drain(send_doubles.at[0], doubles_send)


def one_round(sizes, embeddings, cluster, order, base):
    nz, nx, nc = sizes
    side = nx * nc
    blocks = nz * side
    doubles = blocks // SPARSE
    count, width = embeddings.shape
    pieces = width // LANES
    groups = CLUSTERS // LANES
    vmem = pl.BlockSpec(memory_space=pltpu.VMEM)
    row = jax.ShapeDtypeStruct((1, count), F32)
    dma = pltpu.SemaphoreType.DMA
    inputs = (embeddings, cluster, order)
    if base is None:

        def body(emb_ref, cluster_ref, order_ref, *refs):
            kernel(sizes, emb_ref, cluster_ref, order_ref, None, *refs)

    else:
        inputs += (base,)
        body = functools.partial(kernel, sizes)
    return pl.pallas_call(
        body,
        out_shape=(row, row, jax.ShapeDtypeStruct((1, LANES), F32), row),
        in_specs=[vmem] * len(inputs),
        out_specs=(vmem,) * 4,
        scratch_shapes=[
            pltpu.VMEM((groups, LANES), F32),
            pltpu.VMEM((side, groups, LANES), F32),
            pltpu.VMEM((nz, groups, LANES), F32),
            pltpu.VMEM((1, LANES), F32),
            pltpu.VMEM((1, LANES), F32),
            pltpu.VMEM((blocks, pieces, LANES), BF16),
            pltpu.VMEM((doubles, pieces, LANES), BF16),
            pltpu.VMEM((blocks, LANES), F32),
            pltpu.VMEM((side, nz, LANES), F32),
            pltpu.VMEM((nz, 1, LANES), F32),
            pltpu.VMEM((blocks, pieces, LANES), BF16),
            pltpu.VMEM((blocks, pieces, LANES), BF16),
            pltpu.VMEM((nz, 1, LANES), F32),
            pltpu.VMEM((blocks, LANES), F32),
            pltpu.VMEM((side, nz, LANES), F32),
            pltpu.VMEM((nz, 1, LANES), F32),
            pltpu.VMEM((nz, 1, LANES), F32),
            pltpu.SemaphoreType.REGULAR((nz,)),
            pltpu.SemaphoreType.REGULAR,
            dma((nz,)),
        ]
        + [dma] * 17,
        compiler_params=pltpu.CompilerParams(
            collective_id=0 if base is None else 1, has_side_effects=True
        ),
    )(*inputs)


def per_device(embeddings, assignment, order):
    nz, nx, nc = (lax.axis_size(a) for a in ("rows", "sub", "pair"))
    count = embeddings.shape[0]
    capacity = nz * nx * nc + nz * nx * nc // SPARSE
    sizes = (nz, nx, nc)
    run = functools.partial(
        one_round,
        sizes,
        embeddings,
        assignment.reshape(1, count),
        order.reshape(1, count),
    )
    best, dist, used, _ = run(None)

    def unfinished(state):
        return state[2] < used[0, 0]

    def next_round(state):
        best, dist, base = state
        more_best, more_dist, _, rank = run(jnp.full((1, count), base))
        late = (rank >= base) & (rank < base + capacity)
        return (
            jnp.where(late, more_best, best),
            jnp.where(late, more_dist, dist),
            base + capacity,
        )

    best, dist, _ = lax.while_loop(
        unfinished, next_round, (best, dist, jnp.float32(capacity))
    )
    return best.reshape(count), dist.reshape(count)


def solution(mesh):
    in_specs = (
        P(("groups", "rows", "sub", "pair"), None),
        P(("groups", "rows", "sub", "pair")),
        P(("groups", "rows", "sub", "pair")),
    )
    out_specs = (P(("groups", "rows", "sub", "pair")), P(("groups", "rows", "sub", "pair")))
    return jax.shard_map(
        per_device, mesh=mesh, in_specs=in_specs, out_specs=out_specs, check_vma=False
    )
```

```python
import functools

import jax
import jax.numpy as jnp
from jax import lax
from jax.experimental import pallas as pl
from jax.experimental.pallas import tpu as pltpu
from jax.sharding import PartitionSpec as P

EPSILON = 1e-06
LANES = 128
CLUSTERS = 1024
SLOTS = 2
SPARSE = 4
MESH = pl.DeviceIdType.MESH
F32 = jnp.float32
BF16 = jnp.bfloat16


def iota(shape, dim):
    return lax.broadcasted_iota(jnp.int32, shape, dim)


def drain(ref, sem):
    pltpu.make_async_copy(ref, ref, sem).wait()


def kernel(
    sizes,
    emb_ref,
    cluster_ref,
    order_ref,
    base_ref,
    best_ref,
    dist_ref,
    used_ref,
    rank_ref,
    flags_out,
    flags_in,
    named,
    used_in,
    used_out,
    send_rows,
    send_doubles,
    order_out,
    order_mid,
    send_order,
    got_rows,
    got_doubles,
    got_order,
    answers,
    gathered,
    send_back,
    got_back,
    ready,
    next_in,
    named_recv,
    flag_send,
    flag_recv,
    named_send,
    used_send,
    used_recv,
    rows_send,
    rows_recv,
    doubles_send,
    doubles_recv,
    mid_send,
    mid_recv,
    order_send,
    order_recv,
    answer_send,
    answer_recv,
    back_send,
    back_recv,
):
    nz, nx, nc = sizes
    side = nx * nc
    blocks = nz * side
    doubles = side // SPARSE
    share = LANES // side
    count, width = emb_ref.shape
    pieces = width // LANES
    z = lax.rem(lax.axis_index("rows") + nz - 1, nz)
    x = lax.axis_index("sub")
    c = lax.axis_index("pair")
    xc = x * nc + c
    me = xc * nz + z
    my_place = z * side + xc
    my_double = z * doubles + xc // SPARSE
    is_double = lax.rem(xc, SPARSE) == 0

    def device(tz, txc):
        return {
            "rows": lax.rem(tz + 1, nz),
            "sub": txc // nc,
            "pair": lax.rem(txc, nc),
        }

    def beside(k):
        return lax.rem(xc + k, side)

    def signal(sem, tz, txc):
        pl.semaphore_signal(sem, inc=1, device_id=device(tz, txc), device_id_type=MESH)

    def remote(src, dst, send, recv, tz, txc):
        return pltpu.make_async_remote_copy(
            src_ref=src,
            dst_ref=dst,
            send_sem=send,
            recv_sem=recv,
            device_id=device(tz, txc),
            device_id_type=MESH,
        )

    barrier = pltpu.get_barrier_semaphore()

    @pl.loop(1, side)
    def _(k):
        signal(barrier, z, beside(k))

    @pl.when(z < nz - 1)
    def _():
        signal(barrier, z + 1, xc)

    cluster = cluster_ref[...]
    high = cluster // LANES
    low = cluster - high * LANES
    groups = CLUSTERS // LANES
    is_high = iota((groups, count), 0) == high
    is_low = (iota((LANES, count), 0) == low).astype(F32).astype(BF16)
    flags_out[...] = lax.dot_general(
        is_high.astype(F32).astype(BF16),
        is_low,
        (((1,), (1,)), ((), ())),
        preferred_element_type=F32,
    )

    pl.semaphore_wait(barrier, side - 1 + (z + nz - 1) // nz)

    @pl.when(z > 0)
    def _():
        signal(next_in, z - 1, xc)

    @pl.loop(1, side)
    def _(k):
        remote(flags_out, flags_in.at[xc], flag_send, flag_recv, z, beside(k)).start()

    flags_in[xc] = flags_out[...]

    values = emb_ref[...].astype(F32)
    unit = (
        values * lax.rsqrt(jnp.sum(values * values, axis=1, keepdims=True) + EPSILON)
    ).astype(BF16)

    drain(flags_in.at[pl.ds(0, side - 1)], flag_recv)
    named[z] = jnp.max(flags_in[...], axis=0)

    def pass_on(tz):
        @pl.when(z < nz - 1)
        def _():
            remote(
                named.at[tz], named.at[tz], named_send, named_recv.at[tz], z + 1, xc
            ).start()

    @pl.when(z < nz - 1)
    def _():
        pl.semaphore_wait(next_in, 1)

    @pl.loop(0, z)
    def _(tz):
        drain(named.at[tz], named_recv.at[tz])
        pass_on(tz)
        signal(ready.at[z], tz, xc)

    pass_on(z)

    seen = jnp.zeros((groups, LANES), F32)
    fresh = []
    for tz in range(nz):
        here = jnp.where(z >= tz, named[tz], 0.0)
        fresh.append(jnp.where((here > 0.0) & (seen == 0.0), 1.0, 0.0))
        seen = jnp.maximum(seen, here)
    firsts = jnp.concatenate(fresh, axis=0).astype(BF16)
    levels = nz * groups
    upper = (iota((LANES, LANES), 0) < iota((LANES, LANES), 1)).astype(F32).astype(BF16)
    lower = (iota((levels, levels), 0) > iota((levels, levels), 1)).astype(F32)
    inside = jnp.dot(firsts, upper, preferred_element_type=F32)
    above = jnp.sum(
        jnp.dot(lower.astype(BF16), firsts, preferred_element_type=F32),
        axis=1,
        keepdims=True,
    )
    ranks = inside + above + 1.0
    table = jnp.zeros((groups, LANES), F32)
    for tz in range(nz):
        table += fresh[tz] * ranks[tz * groups : (tz + 1) * groups]

    used = jnp.broadcast_to(jnp.max(table, axis=(0, 1), keepdims=True), used_out.shape)
    used_out[...] = used

    @pl.when(z == nz - 1)
    def _():
        used_in[...] = used

        @pl.loop(0, nz - 1)
        def _(tz):
            remote(used_out, used_in, used_send, used_recv, tz, xc).start()

    tens = jnp.floor(table * (1.0 / 32.0))
    both = jnp.concatenate([tens, table - tens * 32.0], axis=0).astype(BF16)
    found = jnp.dot(both, is_low, preferred_element_type=F32)
    found = found[0:groups] * 32.0 + found[groups:]
    rank = jnp.sum(jnp.where(is_high, found, 0.0), axis=0, keepdims=True) - 1.0
    rank_ref[...] = rank
    slot = rank if base_ref is None else rank - base_ref[...]
    wanted = [
        iota((blocks, count), 0).astype(F32) == slot,
        iota((nz * doubles, count), 0).astype(F32) + float(blocks) == slot,
    ]
    for w, send in zip(wanted, (send_rows, send_doubles)):
        tiles = jnp.dot(w.astype(F32).astype(BF16), unit, preferred_element_type=F32)
        send[...] = tiles.reshape(w.shape[0], pieces, LANES).astype(BF16)
    position = order_ref[...].astype(F32) + 1.0
    line = iota((blocks, count), 0)
    at_row = lax.rem(line, nz)
    column = line // nz
    places = [
        at_row * side + column,
        jnp.where(
            lax.rem(column, SPARSE) == 0,
            blocks + at_row * doubles + column // SPARSE,
            -CLUSTERS,
        ),
    ]
    orders = [
        jnp.sum(jnp.where(p.astype(F32) == slot, position, 0.0), axis=1, keepdims=True)
        for p in places
    ]
    even = lax.rem(iota((blocks, LANES), 1), SLOTS) == 0
    order_out[...] = jnp.where(even, orders[0], orders[1])

    @pl.loop(1, side, unroll=3)
    def _(k):
        remote(
            order_out.at[pl.ds(pl.multiple_of(beside(k) * nz, nz), nz)],
            order_mid.at[xc],
            mid_send,
            mid_recv,
            z,
            beside(k),
        ).start()

    order_mid[xc] = order_out[pl.ds(pl.multiple_of(xc * nz, nz), nz), :]

    def deliver(tz, txc):
        remote(
            send_rows.at[tz * side + txc], got_rows.at[me], rows_send, rows_recv, tz, txc
        ).start()

    def deliver_double(tz, q):
        remote(
            send_doubles.at[tz * doubles + q],
            got_doubles.at[me],
            doubles_send,
            doubles_recv,
            tz,
            q * SPARSE,
        ).start()

    late = z // (nz - nz // 4)

    @pl.loop(0, nz)
    def _(turn):
        away = nz // 2 + ((turn + 1) // 2) * (1 - 2 * lax.rem(turn, 2))
        tz = turn + (lax.rem(z + away, nz) - turn) * late

        @pl.when(tz > z)
        def _():
            pl.semaphore_wait(ready.at[tz], 1)

        @pl.loop(1, side, unroll=5)
        def _(k):
            deliver(tz, beside(k))

        @pl.when(tz != z)
        def _():
            deliver(tz, xc)

            @pl.loop(0, doubles)
            def _(q):
                deliver_double(tz, q)

        @pl.when(tz == z)
        def _():
            @pl.loop(0, doubles)
            def _(q):
                @pl.when(q * SPARSE != xc)
                def _():
                    deliver_double(tz, q)

    drain(order_mid.at[pl.ds(0, side - 1)], mid_recv)
    origin = iota((nz, LANES), 1) // share
    packed = order_mid[side - 1]
    for n in range(side - 1):
        packed = jnp.where(origin == n, order_mid[n], packed)
    send_order[...] = packed.reshape(nz, 1, LANES)

    @pl.loop(0, nz)
    def _(tz):
        @pl.when(tz != z)
        def _():
            remote(
                send_order.at[tz], got_order.at[z], order_send, order_recv, tz, xc
            ).start()

    got_rows[me] = send_rows[my_place]
    got_order[z] = send_order[z]
    drain(got_order.at[pl.ds(0, nz - 1)], order_recv)
    arrived = got_order[...].reshape(nz, LANES)
    kind = lax.rem(iota((blocks, LANES), 1), 2 * SLOTS)

    def judge(s, got):
        rows = got[...].reshape(blocks, width)
        stamps = jnp.concatenate(
            [
                jnp.broadcast_to(
                    arrived[:, n * share + s : n * share + s + 1], (nz, LANES)
                )
                for n in range(side)
            ],
            axis=0,
        )
        mine = stamps[:, 0:1]
        theirs = jnp.transpose(stamps)[0:1, :]
        gram = lax.dot_general(
            rows, rows, (((1,), (1,)), ((), ())), preferred_element_type=F32
        )
        earlier = (theirs > 0.0) & (theirs < mine)
        nearest = jnp.max(jnp.where(earlier, gram, -1.0), axis=1, keepdims=True)
        total = jnp.sum(jnp.where(theirs > 0.0, 1.0, 0.0), axis=1, keepdims=True)
        summed = jnp.dot(
            jnp.ones((8, blocks), BF16), rows, preferred_element_type=F32
        )[0:1]
        offset = rows.astype(F32) - summed / jnp.maximum(total, 1.0)
        apart = jnp.sum(offset * offset, axis=1, keepdims=True)
        return nearest, apart

    drain(got_rows.at[pl.ds(0, blocks - 1)], rows_recv)
    nearest, apart = judge(0, got_rows)
    answers[...] = jnp.where(kind == 0, nearest, apart)

    @pl.when(is_double)
    def _():
        got_doubles[me] = send_doubles[my_double]
        drain(got_doubles.at[pl.ds(0, blocks - 1)], doubles_recv)
        nearest, apart = judge(1, got_doubles)
        answers[...] = jnp.where(
            kind == 2, nearest, jnp.where(kind == 3, apart, answers[...])
        )

    @pl.loop(1, side, unroll=3)
    def _(k):
        remote(
            answers.at[pl.ds(pl.multiple_of(beside(k) * nz, nz), nz)],
            gathered.at[xc],
            answer_send,
            answer_recv,
            z,
            beside(k),
        ).start()

    gathered[xc] = answers[pl.ds(pl.multiple_of(xc * nz, nz), nz), :]
    drain(gathered.at[pl.ds(0, side - 1)], answer_recv)
    source = iota((nz, LANES), 1) // share
    packed = gathered[side - 1]
    for n in range(side - 1):
        packed = jnp.where(source == n, gathered[n], packed)
    send_back[...] = packed.reshape(nz, 1, LANES)

    @pl.loop(0, nz)
    def _(tz):
        @pl.when(tz != z)
        def _():
            remote(
                send_back.at[tz], got_back.at[z], back_send, back_recv, tz, xc
            ).start()

    got_back[z] = send_back[z]
    drain(got_back.at[pl.ds(0, nz - 1)], back_recv)

    back = got_back[...].reshape(nz, LANES)
    columns = jnp.transpose(
        jnp.concatenate([back, jnp.zeros((LANES - nz, LANES), F32)], axis=0)
    )
    double = slot >= float(blocks)
    per_row = jnp.where(double, float(doubles), float(side))
    index = jnp.where(double, slot - float(blocks), slot)
    at_row = jnp.floor(index / per_row)
    step = jnp.where(double, float(SPARSE * share), float(share))
    at_lane = (index - at_row * per_row) * step + jnp.where(double, 2.0, 0.0)
    picked = jnp.zeros((LANES, count), F32)
    for t in range(nz):
        picked = jnp.where(at_row == float(t), columns[:, t : t + 1], picked)
    lane = iota((LANES, count), 0).astype(F32)
    best_ref[...] = jnp.sum(
        jnp.where(lane == at_lane, picked, 0.0), axis=0, keepdims=True
    )
    dist_ref[...] = jnp.sum(
        jnp.where(lane == at_lane + 1.0, picked, 0.0), axis=0, keepdims=True
    )

    @pl.when(z < nz - 1)
    def _():
        drain(used_in, used_recv)

        @pl.loop(0, z + 1)
        def _(tz):
            drain(named.at[tz], named_send)

    @pl.when(z == nz - 1)
    def _():
        @pl.loop(0, nz - 1)
        def _(tz):
            drain(used_out, used_send)

    used_ref[...] = used_in[...]
    drain(flags_in.at[pl.ds(0, side - 1)], flag_send)
    drain(order_mid.at[pl.ds(0, side - 1)], mid_send)
    drain(gathered.at[pl.ds(0, side - 1)], answer_send)
    drain(send_order.at[pl.ds(0, nz - 1)], order_send)
    drain(send_back.at[pl.ds(0, nz - 1)], back_send)
    drain(send_rows.at[pl.ds(0, blocks - 1)], rows_send)
    drain(send_doubles.at[pl.ds(0, nz * doubles - 1)], doubles_send)

    @pl.when(jnp.logical_not(is_double))
    def _():
        drain(send_doubles.at[0], doubles_send)


def one_round(sizes, embeddings, cluster, order, base):
    nz, nx, nc = sizes
    side = nx * nc
    blocks = nz * side
    doubles = blocks // SPARSE
    count, width = embeddings.shape
    pieces = width // LANES
    groups = CLUSTERS // LANES
    vmem = pl.BlockSpec(memory_space=pltpu.VMEM)
    row = jax.ShapeDtypeStruct((1, count), F32)
    dma = pltpu.SemaphoreType.DMA
    inputs = (embeddings, cluster, order)
    if base is None:

        def body(emb_ref, cluster_ref, order_ref, *refs):
            kernel(sizes, emb_ref, cluster_ref, order_ref, None, *refs)

    else:
        inputs += (base,)
        body = functools.partial(kernel, sizes)
    return pl.pallas_call(
        body,
        out_shape=(row, row, jax.ShapeDtypeStruct((1, LANES), F32), row),
        in_specs=[vmem] * len(inputs),
        out_specs=(vmem,) * 4,
        scratch_shapes=[
            pltpu.VMEM((groups, LANES), F32),
            pltpu.VMEM((side, groups, LANES), F32),
            pltpu.VMEM((nz, groups, LANES), F32),
            pltpu.VMEM((1, LANES), F32),
            pltpu.VMEM((1, LANES), F32),
            pltpu.VMEM((blocks, pieces, LANES), BF16),
            pltpu.VMEM((doubles, pieces, LANES), BF16),
            pltpu.VMEM((blocks, LANES), F32),
            pltpu.VMEM((side, nz, LANES), F32),
            pltpu.VMEM((nz, 1, LANES), F32),
            pltpu.VMEM((blocks, pieces, LANES), BF16),
            pltpu.VMEM((blocks, pieces, LANES), BF16),
            pltpu.VMEM((nz, 1, LANES), F32),
            pltpu.VMEM((blocks, LANES), F32),
            pltpu.VMEM((side, nz, LANES), F32),
            pltpu.VMEM((nz, 1, LANES), F32),
            pltpu.VMEM((nz, 1, LANES), F32),
            pltpu.SemaphoreType.REGULAR((nz,)),
            pltpu.SemaphoreType.REGULAR,
            dma((nz,)),
        ]
        + [dma] * 17,
        compiler_params=pltpu.CompilerParams(
            collective_id=0 if base is None else 1, has_side_effects=True
        ),
    )(*inputs)


def per_device(embeddings, assignment, order):
    nz, nx, nc = (lax.axis_size(a) for a in ("rows", "sub", "pair"))
    count = embeddings.shape[0]
    capacity = nz * nx * nc + nz * nx * nc // SPARSE
    sizes = (nz, nx, nc)
    run = functools.partial(
        one_round,
        sizes,
        embeddings,
        assignment.reshape(1, count),
        order.reshape(1, count),
    )
    best, dist, used, _ = run(None)

    def unfinished(state):
        return state[2] < used[0, 0]

    def next_round(state):
        best, dist, base = state
        more_best, more_dist, _, rank = run(jnp.full((1, count), base))
        late = (rank >= base) & (rank < base + capacity)
        return (
            jnp.where(late, more_best, best),
            jnp.where(late, more_dist, dist),
            base + capacity,
        )

    best, dist, _ = lax.while_loop(
        unfinished, next_round, (best, dist, jnp.float32(capacity))
    )
    return best.reshape(count), dist.reshape(count)


def solution(mesh):
    in_specs = (
        P(("groups", "rows", "sub", "pair"), None),
        P(("groups", "rows", "sub", "pair")),
        P(("groups", "rows", "sub", "pair")),
    )
    out_specs = (P(("groups", "rows", "sub", "pair")), P(("groups", "rows", "sub", "pair")))
    return jax.shard_map(
        per_device, mesh=mesh, in_specs=in_specs, out_specs=out_specs, check_vma=False
    )
```
